32 devices in a mesh: rep: 1, dp: 32 (over x, y, z, core).
Axes of the slice: x: 2, y: 2, z: 4, core: 2. Of those that a mesh axis runs over, the one named last changes fastest.
Arguments:
- a: bfloat16 [32, 2, 4096, 1024], P(('rep', 'dp'))
- g: bfloat16 [32, 2, 4096, 3328], P(('rep', 'dp'))
Outputs:
- output: bfloat16 [2, 1024, 3328], P('rep')
All inputs are finite; a program needn't handle non-finite values.
Results may differ from the reference program's by a relative error of at most 0.012.
Values are sent between devices in bfloat16 or wider.
A program may use at most 2 GiB of HBM per device.

```python
import jax
import jax.numpy as jnp
from jax import lax

DEVICES = 32
MATRICES = 2
TOKENS = 4096
D = 1024
FF = 3328


def setup_inputs(seed: int = 0, part: int = 0) -> dict:
    ka, kg, ks = (jax.random.fold_in(k, part) for k in jax.random.split(jax.random.key(seed), 3))
    size = 2.0 ** jax.random.uniform(ks, (DEVICES, MATRICES, 1, 1), jnp.float32, -1.0, 1.0)
    a = jax.random.normal(ka, (DEVICES, MATRICES, TOKENS, D), jnp.float32)
    g = size * jax.random.normal(kg, (DEVICES, MATRICES, TOKENS, FF), jnp.float32) * (DEVICES * TOKENS) ** -0.5
    return {"a": a.astype(jnp.bfloat16), "g": g.astype(jnp.bfloat16)}


def reference(a, g):
    def take(so_far, one):
        return so_far + jnp.einsum("ntd,ntf->ndf", *one, preferred_element_type=jnp.float32), None

    return lax.scan(take, jnp.zeros((MATRICES, D, FF), jnp.float32), (a, g))[0].astype(jnp.bfloat16)
```

```python
import jax
import jax.numpy as jnp
from jax import lax
from jax.experimental import pallas as pl
from jax.experimental.pallas import tpu as pltpu
from jax.sharding import PartitionSpec as P

MESH = pl.DeviceIdType.MESH
MATS, TOKENS, D, FF = 2, 4096, 1024, 3328
COLS = 256
PER = FF // COLS
TILES = MATS * PER
HALF, QUARTER, BLOCK, PIECE = D // 2, D // 4, D // 16, D // 32
ZN = 4
GSLOTS = 3
SLOTS = 4
ZSLOTS = 8
PUTS = 8
AT = dict(a=2, z1=5, z2=8, z3=11, c=14, g0=16, g1=18, g2=21, g3=24, g4=27, g5=31, g6=33)
DN = (((0,), (0,)), ((), ()))


def kernel(
    a_hbm, g_hbm, out, av, gv, own, d_send, d_recv, a_send, a_recv, zsum, zu_send, zd_send, zu_recv, zd_recv,
    c_send, c_keep, c_recv, a_sem, g_sem, ds, dr, xs, xr, us, ur, vs, vr, cs, cr,
    gcs, gcr, gus, gur, gvs, gvr, gas, gar, gds, gdr,
):
    rep, me = lax.axis_index("rep"), lax.axis_index("dp")
    c, z = lax.rem(me, 2), lax.rem(lax.div(me, 2), ZN)
    y, x = lax.rem(lax.div(me, 8), 2), lax.div(me, 16)
    first = jnp.where(c == 0, x, y)
    third = jnp.where(c == 0, y, x)
    over_x, over_y = me + 16 * (1 - 2 * x), me + 8 * (1 - 2 * y)
    first_peer = jnp.where(c == 0, over_x, over_y)
    third_peer = jnp.where(c == 0, over_y, over_x)
    partner, above, below = me + 1 - 2 * c, me + 2, me - 2
    has_above, has_below = z < ZN - 1, z > 0

    def remote(src, dst, send, recv, dev):
        return pltpu.make_async_remote_copy(
            src_ref=src, dst_ref=dst, send_sem=send, recv_sem=recv, device_id=(rep, dev), device_id_type=MESH
        )

    def load_g(t):
        n, j = lax.div(t, PER), lax.rem(t, PER)
        s = lax.rem(t, GSLOTS)
        return pltpu.make_async_copy(
            g_hbm.at[0, n, :, pl.ds(pl.multiple_of(j * COLS, COLS), COLS)], gv.at[s], g_sem.at[s]
        )

    def load_a(k):
        cols = pl.ds(pl.multiple_of(jnp.where(k == 0, 1 - c, c) * HALF, HALF), HALF)
        return pltpu.make_async_copy(a_hbm.at[0, 0, :, cols], av.at[0, :, cols], a_sem.at[k])

    load_rest = pltpu.make_async_copy(a_hbm.at[0, 1], av.at[1], a_sem.at[2])
    load_g(0).start()
    load_a(0).start()
    load_a(1).start()
    load_g(1).start()

    barrier = pltpu.get_barrier_semaphore()
    for dev in (partner, over_x, over_y):
        pl.semaphore_signal(barrier, inc=1, device_id=(rep, dev), device_id_type=MESH)

    @pl.when(has_above)
    def _():
        pl.semaphore_signal(barrier, inc=1, device_id=(rep, above), device_id_type=MESH)

    @pl.when(has_below)
    def _():
        pl.semaphore_signal(barrier, inc=1, device_id=(rep, below), device_id_type=MESH)

    pl.semaphore_wait(barrier, 3 + has_above.astype(jnp.int32) + has_below.astype(jnp.int32))

    def rows(start, size):
        return pl.ds(pl.multiple_of(start, size), size)

    def copy_d(i):
        s = lax.rem(i, SLOTS)
        return remote(d_send.at[s], d_recv.at[i], ds.at[i], dr.at[i], partner)

    def copy_a(i):
        s = lax.rem(i, SLOTS)
        return remote(a_send.at[s], a_recv.at[i], xs.at[i], xr.at[i], first_peer)

    def copy_u(h, i):
        s = lax.rem(i, SLOTS)
        return remote(zu_send.at[h - 1, s], zu_recv.at[h - 1, i], us.at[h - 1, i], ur.at[h - 1, i], above)

    def copy_v(h, i):
        s = lax.rem(i, SLOTS)
        return remote(zd_send.at[h - 1, s], zd_recv.at[h - 1, i], vs.at[h - 1, i], vr.at[h - 1, i], below)

    def copy_c(i):
        s = lax.rem(i, SLOTS)
        return remote(c_send.at[s], c_recv.at[i], cs.at[i], cr.at[i], third_peer)

    def place(i, start, size):
        n, j = lax.div(i, PER), lax.rem(i, PER)
        return out.at[n, rows(start, size), pl.ds(pl.multiple_of(j * COLS, COLS), COLS)]

    def shared(i, start, size, send, recv, dev):
        ref = place(i, start, size)
        return remote(ref, ref, send, recv, dev)

    base_a = c * HALF + first * QUARTER
    base_c = base_a + z * BLOCK

    def copy_gc(i, mine=True):
        return shared(i, base_c + (third if mine else 1 - third) * PIECE, PIECE, gcs.at[i], gcr.at[i], third_peer)

    def copy_gu(k, i, block):
        return shared(i, base_a + block * BLOCK, BLOCK, gus.at[k - 1, i], gur.at[k - 1, i], above)

    def copy_gv(k, i, block):
        return shared(i, base_a + block * BLOCK, BLOCK, gvs.at[k - 1, i], gvr.at[k - 1, i], below)

    def copy_ga(i, mine=True):
        return shared(
            i, c * HALF + (first if mine else 1 - first) * QUARTER, QUARTER, gas.at[i], gar.at[i], first_peer
        )

    def copy_gd(i, mine=True):
        return shared(i, (c if mine else 1 - c) * HALF, HALF, gds.at[i], gdr.at[i], partner)

    def reuse(copy, i):
        @pl.when(i >= SLOTS)
        def _():
            copy(i - SLOTS).wait_send()

    def step_a(i):
        s, zs = lax.rem(i, SLOTS), lax.rem(i, ZSLOTS)
        copy_d(i).wait_recv()
        reuse(copy_a, i)
        away, keep = rows((1 - first) * QUARTER, QUARTER), rows(first * QUARTER, QUARTER)
        a_send[s] = (own[away, :] + d_recv[i, away, :].astype(jnp.float32)).astype(jnp.bfloat16)
        copy_a(i).start()
        zsum[zs] = own[keep, :] + d_recv[i, keep, :].astype(jnp.float32)

    def hop(h, i):
        s, zs = lax.rem(i, SLOTS), lax.rem(i, ZSLOTS)
        if h == 1:
            copy_a(i).wait_recv()
            zsum[zs] += a_recv[i].astype(jnp.float32)
        else:
            take(h - 1, i)
        if h == ZN:
            return

        @pl.when(jnp.logical_and(has_above, z <= h - 1))
        def _():
            reuse(lambda k: copy_u(h, k), i)
            zu_send[h - 1, s] = zsum[zs, rows((z + ZN - h) * BLOCK, BLOCK), :].astype(jnp.bfloat16)
            copy_u(h, i).start()

        @pl.when(jnp.logical_and(has_below, z >= ZN - h))
        def _():
            reuse(lambda k: copy_v(h, k), i)
            zd_send[h - 1, s] = zsum[zs, rows((z - ZN + h) * BLOCK, BLOCK), :].astype(jnp.bfloat16)
            copy_v(h, i).start()

    def take(h, i):
        zs = lax.rem(i, ZSLOTS)

        @pl.when(jnp.logical_and(has_below, z <= h))
        def _():
            copy_u(h, i).wait_recv()
            zsum[zs, rows((z + ZN - 1 - h) * BLOCK, BLOCK), :] += zu_recv[h - 1, i].astype(jnp.float32)

        @pl.when(jnp.logical_and(has_above, z >= ZN - 1 - h))
        def _():
            copy_v(h, i).wait_recv()
            zsum[zs, rows((z - ZN + 1 + h) * BLOCK, BLOCK), :] += zd_recv[h - 1, i].astype(jnp.float32)

    def step_c(i):
        s, zs = lax.rem(i, SLOTS), lax.rem(i, ZSLOTS)
        take(ZN - 1, i)
        reuse(copy_c, i)
        c_send[s] = zsum[zs, rows(z * BLOCK + (1 - third) * PIECE, PIECE), :].astype(jnp.bfloat16)
        copy_c(i).start()
        c_keep[s] = zsum[zs, rows(z * BLOCK + third * PIECE, PIECE), :]

    def step_g0(i):
        s = lax.rem(i, SLOTS)
        copy_c(i).wait_recv()
        total = c_keep[s] + c_recv[i].astype(jnp.float32)
        n, j = lax.div(i, PER), lax.rem(i, PER)
        out[n, rows(base_c + third * PIECE, PIECE), pl.ds(pl.multiple_of(j * COLS, COLS), COLS)] = total.astype(
            jnp.bfloat16
        )
        copy_gc(i).start()

    def spread(k, i):
        if k == 1:
            copy_gc(i, False).wait_recv()
        else:
            arrive(k - 1, i)

        @pl.when(jnp.logical_and(has_above, z >= k - 1))
        def _():
            copy_gu(k, i, z - k + 1).start()

        @pl.when(jnp.logical_and(has_below, z <= ZN - k))
        def _():
            copy_gv(k, i, z + k - 1).start()

    def arrive(k, i):
        @pl.when(z >= k)
        def _():
            copy_gu(k, i, z - k).wait_recv()

        @pl.when(z <= ZN - 1 - k)
        def _():
            copy_gv(k, i, z + k).wait_recv()

    def step_g4(i):
        arrive(ZN - 1, i)
        copy_ga(i).start()

    def step_g5(i):
        copy_ga(i, False).wait_recv()
        copy_gd(i).start()

    def step_g6(i):
        copy_gd(i, False).wait_recv()

    steps = dict(
        a=step_a,
        z1=lambda i: hop(1, i),
        z2=lambda i: hop(2, i),
        z3=lambda i: hop(3, i),
        c=step_c,
        g0=step_g0,
        g1=lambda i: spread(1, i),
        g2=lambda i: spread(2, i),
        g3=lambda i: spread(3, i),
        g4=step_g4,
        g5=step_g5,
        g6=step_g6,
    )
    order = sorted(steps, key=lambda name: -AT[name])

    def run(t, parity):
        for name in order:
            if AT[name] % 2 == parity:
                i = t - AT[name] // 2

                @pl.when(jnp.logical_and(i >= 0, i < TILES))
                def _():
                    steps[name](i)

    def loop(t, carry):
        run(t, 0)
        live = t < TILES
        n = lax.div(t, PER)
        gs = lax.rem(t, GSLOTS)

        @pl.when(live)
        def _():
            @pl.when(t + 2 < TILES)
            def _():
                load_g(t + 2).start()

            @pl.when(t == 2)
            def _():
                load_rest.start()

            @pl.when(t == PER)
            def _():
                load_rest.wait()

            load_g(t).wait()

            @pl.when(t == 0)
            def _():
                load_a(0).wait()

            reuse(copy_d, t)
            d_send[lax.rem(t, SLOTS)] = lax.dot_general(
                av[n, :, pl.ds(pl.multiple_of((1 - c) * HALF, HALF), HALF)],
                gv[gs],
                DN,
                preferred_element_type=jnp.float32,
            ).astype(jnp.bfloat16)
            copy_d(t).start()

        run(t, 1)

        @pl.when(live)
        def _():
            @pl.when(t == 0)
            def _():
                load_a(1).wait()

            own[...] = lax.dot_general(
                av[n, :, pl.ds(pl.multiple_of(c * HALF, HALF), HALF)],
                gv[gs],
                DN,
                preferred_element_type=jnp.float32,
            )

        return carry

    lax.fori_loop(0, TILES + max(AT.values()) // 2, loop, 0)

    def finish_staged(i, carry):
        copy_d(i).wait_send()
        copy_a(i).wait_send()
        copy_c(i).wait_send()
        for h in range(1, ZN):

            @pl.when(jnp.logical_and(has_above, z <= h - 1))
            def _():
                copy_u(h, i).wait_send()

            @pl.when(jnp.logical_and(has_below, z >= ZN - h))
            def _():
                copy_v(h, i).wait_send()

        return carry

    def finish_shared(i, carry):
        copy_gc(i).wait_send()
        copy_ga(i).wait_send()
        copy_gd(i).wait_send()
        for k in range(1, ZN):

            @pl.when(jnp.logical_and(has_above, z >= k - 1))
            def _():
                copy_gu(k, i, z - k + 1).wait_send()

            @pl.when(jnp.logical_and(has_below, z <= ZN - k))
            def _():
                copy_gv(k, i, z + k - 1).wait_send()

        return carry

    lax.fori_loop(TILES - SLOTS, TILES, finish_staged, 0)
    lax.fori_loop(0, TILES, finish_shared, 0)


def put(sums, out, sem):
    copies = []
    for k in range(MATS * PUTS):
        part = (k // PUTS, pl.ds(k % PUTS * (D // PUTS), D // PUTS))
        copies.append(pltpu.make_async_copy(sums.at[part], out.at[part], sem.at[k]))
        copies[-1].start()
    for copy in copies:
        copy.wait()


def solution(mesh):
    bf16, f32 = jnp.bfloat16, jnp.float32

    def step(a, g):
        dma = pltpu.SemaphoreType.DMA
        one, three = dma((TILES,)), dma((ZN - 1, TILES))
        scratch = [
            pltpu.VMEM((MATS, TOKENS, D), bf16),
            pltpu.VMEM((GSLOTS, TOKENS, COLS), bf16),
            pltpu.VMEM((HALF, COLS), f32),
            pltpu.VMEM((SLOTS, HALF, COLS), bf16),
            pltpu.VMEM((TILES, HALF, COLS), bf16),
            pltpu.VMEM((SLOTS, QUARTER, COLS), bf16),
            pltpu.VMEM((TILES, QUARTER, COLS), bf16),
            pltpu.VMEM((ZSLOTS, QUARTER, COLS), f32),
            pltpu.VMEM((ZN - 1, SLOTS, BLOCK, COLS), bf16),
            pltpu.VMEM((ZN - 1, SLOTS, BLOCK, COLS), bf16),
            pltpu.VMEM((ZN - 1, TILES, BLOCK, COLS), bf16),
            pltpu.VMEM((ZN - 1, TILES, BLOCK, COLS), bf16),
            pltpu.VMEM((SLOTS, PIECE, COLS), bf16),
            pltpu.VMEM((SLOTS, PIECE, COLS), f32),
            pltpu.VMEM((TILES, PIECE, COLS), bf16),
            dma((3,)),
            dma((GSLOTS,)),
        ]
        scratch += [one] * 4 + [three] * 4 + [one] * 2
        scratch += [one] * 2 + [three] * 4 + [one] * 4
        sums = pl.pallas_call(
            kernel,
            out_shape=pltpu.VMEM((MATS, D, FF), bf16),
            in_specs=[pl.BlockSpec(memory_space=pl.ANY)] * 2,
            out_specs=pl.BlockSpec(memory_space=pltpu.VMEM),
            scratch_shapes=scratch,
            compiler_params=pltpu.CompilerParams(
                collective_id=0, has_side_effects=True, vmem_limit_bytes=48 * 2**20
            ),
        )(a, g)
        return pl.pallas_call(
            put,
            out_shape=jax.ShapeDtypeStruct((MATS, D, FF), bf16),
            in_specs=[pl.BlockSpec(memory_space=pltpu.VMEM)],
            out_specs=pl.BlockSpec(memory_space=pl.ANY),
            scratch_shapes=[dma((MATS * PUTS,))],
            compiler_params=pltpu.CompilerParams(vmem_limit_bytes=2**20),
        )(sums)

    return jax.shard_map(
        step,
        mesh=mesh,
        in_specs=(P(("rep", "dp")), P(("rep", "dp"))),
        out_specs=P("rep"),
        check_vma=False,
    )
```

```python
import jax
import jax.numpy as jnp
from jax import lax
from jax.experimental import pallas as pl
from jax.experimental.pallas import tpu as pltpu
from jax.sharding import PartitionSpec as P

MESH = pl.DeviceIdType.MESH
MATS, TOKENS, D, FF = 2, 4096, 1024, 3328
COLS = 256
PER = FF // COLS
PARTS = 1
TILES = MATS * PER * PARTS
CORE = D // 2
HALF = CORE // PARTS
QUARTER, BLOCK, PIECE = HALF // 2, HALF // 8, HALF // 16
ZN = 4
GSLOTS = 3
SLOTS = 8
LATE = 32
ZSLOTS = 12
PUTS = 8
AT = dict(a=2, z1=4, z2=5, z3=7, c=9, g0=11, g1=13, g2=15, g3=17, g4=19, g5=29)
DN = (((0,), (0,)), ((), ()))


def kernel(
    a_hbm, g_hbm, out, av, gv, own, d_send, d_recv, a_send, a_recv, zsum, zu_send, zd_send, zu_recv, zd_recv,
    c_send, c_keep, c_recv, a_sem, g_sem, ds, dr, xs, xr, us, ur, vs, vr, cs, cr,
    gcs, gcr, gus, gur, gvs, gvr, gas, gar, gds, gdr,
):
    rep, me = lax.axis_index("rep"), lax.axis_index("dp")
    c, z = lax.rem(me, 2), lax.rem(lax.div(me, 2), ZN)
    y, x = lax.rem(lax.div(me, 8), 2), lax.div(me, 16)
    first = jnp.where(c == 0, x, y)
    third = jnp.where(c == 0, y, x)
    over_x, over_y = me + 16 * (1 - 2 * x), me + 8 * (1 - 2 * y)
    first_peer = jnp.where(c == 0, over_x, over_y)
    third_peer = jnp.where(c == 0, over_y, over_x)
    partner, above, below = me + 1 - 2 * c, me + 2, me - 2
    has_above, has_below = z < ZN - 1, z > 0

    def remote(src, dst, send, recv, dev):
        return pltpu.make_async_remote_copy(
            src_ref=src, dst_ref=dst, send_sem=send, recv_sem=recv, device_id=(rep, dev), device_id_type=MESH
        )

    def load_g(u):
        n, j = lax.div(u, PER), lax.rem(u, PER)
        s = lax.rem(u, GSLOTS)
        return pltpu.make_async_copy(
            g_hbm.at[0, n, :, pl.ds(pl.multiple_of(j * COLS, COLS), COLS)], gv.at[s], g_sem.at[s]
        )

    def load_a(n, k):
        cols = pl.ds(pl.multiple_of((1 - c if k == 0 else c) * CORE, CORE), CORE)
        return pltpu.make_async_copy(
            a_hbm.at[0, n, :, cols], av.at[n, :, k * CORE : (k + 1) * CORE], a_sem.at[n, k]
        )

    load_g(0).start()
    load_a(0, 0).start()
    load_a(0, 1).start()
    load_g(1).start()

    barrier = pltpu.get_barrier_semaphore()
    for dev in (partner, over_x, over_y):
        pl.semaphore_signal(barrier, inc=1, device_id=(rep, dev), device_id_type=MESH)

    @pl.when(has_above)
    def _():
        pl.semaphore_signal(barrier, inc=1, device_id=(rep, above), device_id_type=MESH)

    @pl.when(has_below)
    def _():
        pl.semaphore_signal(barrier, inc=1, device_id=(rep, below), device_id_type=MESH)

    pl.semaphore_wait(barrier, 3 + has_above.astype(jnp.int32) + has_below.astype(jnp.int32))

    def rows(start, size):
        return pl.ds(pl.multiple_of(start, size), size)

    def copy_d(i):
        s = lax.rem(i, SLOTS)
        return remote(d_send.at[s], d_recv.at[i], ds.at[s], dr.at[s], partner)

    def copy_a(i):
        s = lax.rem(i, SLOTS)
        return remote(a_send.at[s], a_recv.at[i], xs.at[s], xr.at[s], first_peer)

    def copy_u(h, i):
        s = lax.rem(i, SLOTS)
        return remote(zu_send.at[h - 1, s], zu_recv.at[h - 1, i], us.at[h - 1, s], ur.at[h - 1, s], above)

    def copy_v(h, i):
        s = lax.rem(i, SLOTS)
        return remote(zd_send.at[h - 1, s], zd_recv.at[h - 1, i], vs.at[h - 1, s], vr.at[h - 1, s], below)

    def copy_c(i):
        s = lax.rem(i, SLOTS)
        return remote(c_send.at[s], c_recv.at[i], cs.at[s], cr.at[s], third_peer)

    def spot(i):
        n, j = lax.div(i, PER * PARTS), lax.rem(lax.div(i, PARTS), PER)
        return n, lax.rem(i, PARTS) * HALF, pl.ds(pl.multiple_of(j * COLS, COLS), COLS)

    def place(i, start, size):
        n, row, cols = spot(i)
        return out.at[n, rows(row + start, size), cols]

    def shared(i, start, size, send, recv, dev):
        ref = place(i, start, size)
        return remote(ref, ref, send, recv, dev)

    base_a = c * CORE + first * QUARTER
    base_c = base_a + z * BLOCK

    def copy_gc(i, mine=True):
        return shared(i, base_c + (third if mine else 1 - third) * PIECE, PIECE, gcs, gcr.at[lax.rem(i, SLOTS)], third_peer)

    def copy_gu(k, i, block):
        return shared(i, base_a + block * BLOCK, BLOCK, gus.at[k - 1], gur.at[k - 1, lax.rem(i, SLOTS)], above)

    def copy_gv(k, i, block):
        return shared(i, base_a + block * BLOCK, BLOCK, gvs.at[k - 1], gvr.at[k - 1, lax.rem(i, SLOTS)], below)

    def copy_ga(i, mine=True):
        return shared(
            i, c * CORE + (first if mine else 1 - first) * QUARTER, QUARTER, gas, gar.at[lax.rem(i, LATE)], first_peer
        )

    def copy_gd(i, mine=True):
        return shared(i, (c if mine else 1 - c) * CORE, HALF, gds, gdr, partner)

    def reuse(copy, i):
        @pl.when(i >= SLOTS)
        def _():
            copy(i - SLOTS).wait_send()

    def step_a(i):
        s, zs = lax.rem(i, SLOTS), lax.rem(i, ZSLOTS)
        o = lax.rem(i, 2)
        copy_d(i).wait_recv()
        reuse(copy_a, i)
        away, keep = rows((1 - first) * QUARTER, QUARTER), rows(first * QUARTER, QUARTER)
        a_send[s] = (own[o, away, :] + d_recv[i, away, :].astype(jnp.float32)).astype(jnp.bfloat16)
        copy_a(i).start()
        zsum[zs] = own[o, keep, :] + d_recv[i, keep, :].astype(jnp.float32)

    def hop(h, i):
        s, zs = lax.rem(i, SLOTS), lax.rem(i, ZSLOTS)
        if h == 1:
            copy_a(i).wait_recv()
            zsum[zs] += a_recv[i].astype(jnp.float32)
        else:
            take(h - 1, i)
        if h == ZN:
            return

        @pl.when(jnp.logical_and(has_above, z <= h - 1))
        def _():
            reuse(lambda k: copy_u(h, k), i)
            zu_send[h - 1, s] = zsum[zs, rows((z + ZN - h) * BLOCK, BLOCK), :].astype(jnp.bfloat16)
            copy_u(h, i).start()

        @pl.when(jnp.logical_and(has_below, z >= ZN - h))
        def _():
            reuse(lambda k: copy_v(h, k), i)
            zd_send[h - 1, s] = zsum[zs, rows((z - ZN + h) * BLOCK, BLOCK), :].astype(jnp.bfloat16)
            copy_v(h, i).start()

    def take(h, i):
        zs = lax.rem(i, ZSLOTS)

        @pl.when(jnp.logical_and(has_below, z <= h))
        def _():
            copy_u(h, i).wait_recv()
            zsum[zs, rows((z + ZN - 1 - h) * BLOCK, BLOCK), :] += zu_recv[h - 1, i].astype(jnp.float32)

        @pl.when(jnp.logical_and(has_above, z >= ZN - 1 - h))
        def _():
            copy_v(h, i).wait_recv()
            zsum[zs, rows((z - ZN + 1 + h) * BLOCK, BLOCK), :] += zd_recv[h - 1, i].astype(jnp.float32)

    def step_c(i):
        s, zs = lax.rem(i, SLOTS), lax.rem(i, ZSLOTS)
        take(ZN - 1, i)
        reuse(copy_c, i)
        c_send[s] = zsum[zs, rows(z * BLOCK + (1 - third) * PIECE, PIECE), :].astype(jnp.bfloat16)
        copy_c(i).start()
        c_keep[s] = zsum[zs, rows(z * BLOCK + third * PIECE, PIECE), :]

    def step_g0(i):
        s = lax.rem(i, SLOTS)
        copy_c(i).wait_recv()
        total = c_keep[s] + c_recv[i].astype(jnp.float32)
        n, row, cols = spot(i)
        out[n, rows(row + base_c + third * PIECE, PIECE), cols] = total.astype(jnp.bfloat16)
        copy_gc(i).start()

    def spread(k, i):
        if k == 1:
            copy_gc(i, False).wait_recv()
        else:
            arrive(k - 1, i)

        @pl.when(jnp.logical_and(has_above, z >= k - 1))
        def _():
            copy_gu(k, i, z - k + 1).start()

        @pl.when(jnp.logical_and(has_below, z <= ZN - k))
        def _():
            copy_gv(k, i, z + k - 1).start()

    def arrive(k, i):
        @pl.when(z >= k)
        def _():
            copy_gu(k, i, z - k).wait_recv()

        @pl.when(z <= ZN - 1 - k)
        def _():
            copy_gv(k, i, z + k).wait_recv()

    def step_g4(i):
        arrive(ZN - 1, i)
        copy_ga(i).start()

    def step_g5(i):
        copy_ga(i, False).wait_recv()
        copy_gd(i).start()

    steps = dict(
        a=step_a,
        z1=lambda i: hop(1, i),
        z2=lambda i: hop(2, i),
        z3=lambda i: hop(3, i),
        c=step_c,
        g0=step_g0,
        g1=lambda i: spread(1, i),
        g2=lambda i: spread(2, i),
        g3=lambda i: spread(3, i),
        g4=step_g4,
        g5=step_g5,
    )
    order = sorted(steps, key=lambda name: -AT[name])

    def run(t):
        for name in order:
            i = t - AT[name]

            @pl.when(jnp.logical_and(i >= 0, i < TILES))
            def _():
                steps[name](i)

    def compute(u, part):
        n, gs = lax.div(u, PER), lax.rem(u, GSLOTS)
        t = u * PARTS + part
        if part == 0:

            @pl.when(u + 2 < MATS * PER)
            def _():
                load_g(u + 2).start()

            @pl.when(u == 2)
            def _():
                load_a(1, 0).start()
                load_a(1, 1).start()

            load_g(u).wait()

            @pl.when(jnp.logical_or(u == 0, u == PER))
            def _():
                load_a(n, 0).wait()
                load_a(n, 1).wait()

        reuse(copy_d, t)

        def term(half):
            cols = slice(half * CORE + part * HALF, half * CORE + (part + 1) * HALF)
            return lax.dot_general(av[n, :, cols], gv[gs], DN, preferred_element_type=jnp.float32)

        d_send[lax.rem(t, SLOTS)] = term(0).astype(jnp.bfloat16)
        own[lax.rem(u, 2)] = term(1)
        copy_d(t).start()

    def loop(u, carry):
        for part in range(PARTS):
            run(u * PARTS + part)
            pl.when(u < MATS * PER)(lambda part=part: compute(u, part))
        return carry

    lax.fori_loop(0, (TILES + max(AT.values()) + PARTS - 1) // PARTS, loop, 0)

    def finish_staged(i, carry):
        copy_d(i).wait_send()
        copy_a(i).wait_send()
        copy_c(i).wait_send()
        for h in range(1, ZN):

            @pl.when(jnp.logical_and(has_above, z <= h - 1))
            def _():
                copy_u(h, i).wait_send()

            @pl.when(jnp.logical_and(has_below, z >= ZN - h))
            def _():
                copy_v(h, i).wait_send()

        return carry

    lax.fori_loop(TILES - SLOTS, TILES, finish_staged, 0)

    def all_of(size, send, recv, dev):
        ref = out.at[:, 0:size, :]
        return remote(ref, ref, send, recv, dev)

    all_of(PARTS * PIECE, gcs, gdr, third_peer).wait_send()
    all_of(PARTS * QUARTER, gas, gdr, first_peer).wait_send()
    for k in range(1, ZN):

        @pl.when(jnp.logical_and(has_above, z >= k - 1))
        def _():
            all_of(PARTS * BLOCK, gus.at[k - 1], gdr, above).wait_send()

        @pl.when(jnp.logical_and(has_below, z <= ZN - k))
        def _():
            all_of(PARTS * BLOCK, gvs.at[k - 1], gdr, below).wait_send()

    all_of(PARTS * HALF, gds, gdr, partner).wait()


def put(sums, out, sem):
    copies = []
    for k in range(MATS * PUTS):
        part = (k // PUTS, pl.ds(k % PUTS * (D // PUTS), D // PUTS))
        copies.append(pltpu.make_async_copy(sums.at[part], out.at[part], sem.at[k]))
        copies[-1].start()
    for copy in copies:
        copy.wait()


def solution(mesh):
    bf16, f32 = jnp.bfloat16, jnp.float32

    def step(a, g):
        dma = pltpu.SemaphoreType.DMA
        one, three = dma((SLOTS,)), dma((ZN - 1, SLOTS))
        scratch = [
            pltpu.VMEM((MATS, TOKENS, D), bf16),
            pltpu.VMEM((GSLOTS, TOKENS, COLS), bf16),
            pltpu.VMEM((2, HALF, COLS), f32),
            pltpu.VMEM((SLOTS, HALF, COLS), bf16),
            pltpu.VMEM((TILES, HALF, COLS), bf16),
            pltpu.VMEM((SLOTS, QUARTER, COLS), bf16),
            pltpu.VMEM((TILES, QUARTER, COLS), bf16),
            pltpu.VMEM((ZSLOTS, QUARTER, COLS), f32),
            pltpu.VMEM((ZN - 1, SLOTS, BLOCK, COLS), bf16),
            pltpu.VMEM((ZN - 1, SLOTS, BLOCK, COLS), bf16),
            pltpu.VMEM((ZN - 1, TILES, BLOCK, COLS), bf16),
            pltpu.VMEM((ZN - 1, TILES, BLOCK, COLS), bf16),
            pltpu.VMEM((SLOTS, PIECE, COLS), bf16),
            pltpu.VMEM((SLOTS, PIECE, COLS), f32),
            pltpu.VMEM((TILES, PIECE, COLS), bf16),
            dma((MATS, 2)),
            dma((GSLOTS,)),
        ]
        scratch += [one] * 4 + [three] * 4 + [one] * 2
        hops = dma((ZN - 1,))
        scratch += [dma, one, hops, three, hops, three, dma, dma((LATE,)), dma, dma]
        sums = pl.pallas_call(
            kernel,
            out_shape=pltpu.VMEM((MATS, D, FF), bf16),
            in_specs=[pl.BlockSpec(memory_space=pl.ANY)] * 2,
            out_specs=pl.BlockSpec(memory_space=pltpu.VMEM),
            scratch_shapes=scratch,
            compiler_params=pltpu.CompilerParams(
                collective_id=0, has_side_effects=True, vmem_limit_bytes=48 * 2**20
            ),
        )(a, g)
        return pl.pallas_call(
            put,
            out_shape=jax.ShapeDtypeStruct((MATS, D, FF), bf16),
            in_specs=[pl.BlockSpec(memory_space=pltpu.VMEM)],
            out_specs=pl.BlockSpec(memory_space=pl.ANY),
            scratch_shapes=[dma((MATS * PUTS,))],
            compiler_params=pltpu.CompilerParams(vmem_limit_bytes=2**20),
        )(sums)

    return jax.shard_map(
        step,
        mesh=mesh,
        in_specs=(P(("rep", "dp")), P(("rep", "dp"))),
        out_specs=P("rep"),
        check_vma=False,
    )
```

```python
import jax
import jax.numpy as jnp
from jax import lax
from jax.experimental import pallas as pl
from jax.experimental.pallas import tpu as pltpu
from jax.sharding import PartitionSpec as P

MESH = pl.DeviceIdType.MESH
MATS, TOKENS, D, FF = 2, 4096, 1024, 3328
COLS = 256
PER = FF // COLS
TILES = MATS * PER
HALF = D // 2
PIECES = 4
STEP = TOKENS // PIECES
QUARTER, BLOCK, PIECE = HALF // 2, HALF // 8, HALF // 16
ZN = 4
GSLOTS = 3
SLOTS = 6
LATE = 12
ZSLOTS = 9
PUTS = 8
AT = dict(a=3, z1=7, z2=10, z3=13, c=16, g0=19, g1=22, g2=25, g3=29, g4=32, g5=40)
DN = (((0,), (0,)), ((), ()))


def kernel(
    a_hbm, g_hbm, out, av, gv, own, d_send, d_recv, a_send, a_recv, zsum, zu_send, zd_send, zu_recv, zd_recv,
    c_send, c_keep, c_recv, a_sem, g_sem, first_sem, ds, dr, xs, xr, us, ur, vs, vr, cs, cr,
    gcs, gcr, gus, gur, gvs, gvr, gas, gar, gds, gdr,
):
    rep, me = lax.axis_index("rep"), lax.axis_index("dp")
    c, z = lax.rem(me, 2), lax.rem(lax.div(me, 2), ZN)
    y, x = lax.rem(lax.div(me, 8), 2), lax.div(me, 16)
    first = jnp.where(c == 0, x, y)
    third = jnp.where(c == 0, y, x)
    over_x, over_y = me + 16 * (1 - 2 * x), me + 8 * (1 - 2 * y)
    first_peer = jnp.where(c == 0, over_x, over_y)
    third_peer = jnp.where(c == 0, over_y, over_x)
    partner, above, below = me + 1 - 2 * c, me + 2, me - 2
    has_above, has_below = z < ZN - 1, z > 0

    def remote(src, dst, send, recv, dev):
        return pltpu.make_async_remote_copy(
            src_ref=src, dst_ref=dst, send_sem=send, recv_sem=recv, device_id=(rep, dev), device_id_type=MESH
        )

    def load_g(u):
        n, j = lax.div(u, PER), lax.rem(u, PER)
        s = lax.rem(u, GSLOTS)
        return pltpu.make_async_copy(
            g_hbm.at[0, n, :, pl.ds(pl.multiple_of(j * COLS, COLS), COLS)], gv.at[s], g_sem.at[s]
        )

    def load_a(k):
        cols = pl.ds(pl.multiple_of((1 - c if k == 0 else c) * HALF, HALF), HALF)
        return pltpu.make_async_copy(a_hbm.at[0, 1, :, cols], av.at[1, :, k * HALF : (k + 1) * HALF], a_sem.at[k])

    def load_first(p):
        tokens = pl.ds(pl.multiple_of(p * STEP, STEP), STEP)
        copies = [pltpu.make_async_copy(g_hbm.at[0, 0, tokens, 0:COLS], gv.at[0, tokens, :], first_sem.at[2, p])]
        for k in range(2):
            cols = pl.ds(pl.multiple_of((1 - c if k == 0 else c) * HALF, HALF), HALF)
            copies.append(
                pltpu.make_async_copy(
                    a_hbm.at[0, 0, tokens, cols], av.at[0, tokens, k * HALF : (k + 1) * HALF], first_sem.at[k, p]
                )
            )
        return copies

    for copy in load_first(0) + load_first(1):
        copy.start()

    barrier = pltpu.get_barrier_semaphore()
    for dev in (partner, over_x, over_y):
        pl.semaphore_signal(barrier, inc=1, device_id=(rep, dev), device_id_type=MESH)

    @pl.when(has_above)
    def _():
        pl.semaphore_signal(barrier, inc=1, device_id=(rep, above), device_id_type=MESH)

    @pl.when(has_below)
    def _():
        pl.semaphore_signal(barrier, inc=1, device_id=(rep, below), device_id_type=MESH)


    def rows(start, size):
        return pl.ds(pl.multiple_of(start, size), size)

    own[...] = jnp.zeros_like(own)

    def piece(k, carry):
        for copy in load_first(k):
            copy.wait()

        @pl.when(k + 2 < PIECES)
        def _():
            for copy in load_first(k + 2):
                copy.start()

        @pl.when(k == 1)
        def _():
            load_g(1).start()

        tokens = rows(k * STEP, STEP)
        for slot, mine in ((1, 0), (0, 1)):
            own[slot] += lax.dot_general(
                av[0, tokens, mine * HALF : (mine + 1) * HALF],
                gv[0, tokens, :],
                DN,
                preferred_element_type=jnp.float32,
            )
        return carry

    lax.fori_loop(0, PIECES, piece, 0)
    d_send[0] = own[1].astype(jnp.bfloat16)

    pl.semaphore_wait(barrier, 3 + has_above.astype(jnp.int32) + has_below.astype(jnp.int32))

    def copy_d(i):
        s = lax.rem(i, SLOTS)
        return remote(d_send.at[s], d_recv.at[i], ds.at[s], dr.at[s], partner)

    def copy_a(i):
        s = lax.rem(i, SLOTS)
        return remote(a_send.at[s], a_recv.at[i], xs.at[s], xr.at[s], first_peer)

    def copy_u(h, i):
        s = lax.rem(i, SLOTS)
        return remote(zu_send.at[h - 1, s], zu_recv.at[h - 1, i], us.at[h - 1, s], ur.at[h - 1, s], above)

    def copy_v(h, i):
        s = lax.rem(i, SLOTS)
        return remote(zd_send.at[h - 1, s], zd_recv.at[h - 1, i], vs.at[h - 1, s], vr.at[h - 1, s], below)

    def copy_c(i):
        s = lax.rem(i, SLOTS)
        return remote(c_send.at[s], c_recv.at[i], cs.at[s], cr.at[s], third_peer)

    def spot(i):
        n, j = lax.div(i, PER), lax.rem(i, PER)
        return n, pl.ds(pl.multiple_of(j * COLS, COLS), COLS)

    def place(i, start, size):
        n, cols = spot(i)
        return out.at[n, rows(start, size), cols]

    def shared(i, start, size, send, recv, dev):
        ref = place(i, start, size)
        return remote(ref, ref, send, recv, dev)

    base_a = c * HALF + first * QUARTER
    base_c = base_a + z * BLOCK

    def copy_gc(i, mine=True):
        return shared(i, base_c + (third if mine else 1 - third) * PIECE, PIECE, gcs, gcr.at[lax.rem(i, SLOTS)], third_peer)

    def copy_gu(k, i, block):
        return shared(i, base_a + block * BLOCK, BLOCK, gus.at[k - 1], gur.at[k - 1, lax.rem(i, SLOTS)], above)

    def copy_gv(k, i, block):
        return shared(i, base_a + block * BLOCK, BLOCK, gvs.at[k - 1], gvr.at[k - 1, lax.rem(i, SLOTS)], below)

    def copy_ga(i, mine=True):
        return shared(
            i, c * HALF + (first if mine else 1 - first) * QUARTER, QUARTER, gas, gar.at[lax.rem(i, LATE)], first_peer
        )

    def copy_gd(i, mine=True):
        return shared(i, (c if mine else 1 - c) * HALF, HALF, gds, gdr, partner)

    def reuse(copy, i):
        @pl.when(i >= SLOTS)
        def _():
            copy(i - SLOTS).wait_send()

    def step_a(i):
        s, zs = lax.rem(i, SLOTS), lax.rem(i, ZSLOTS)
        o = lax.rem(i, 2)
        copy_d(i).wait_recv()
        reuse(copy_a, i)
        away, keep = rows((1 - first) * QUARTER, QUARTER), rows(first * QUARTER, QUARTER)
        a_send[s] = (own[o, away, :] + d_recv[i, away, :].astype(jnp.float32)).astype(jnp.bfloat16)
        copy_a(i).start()
        zsum[zs] = own[o, keep, :] + d_recv[i, keep, :].astype(jnp.float32)

    def hop(h, i):
        s, zs = lax.rem(i, SLOTS), lax.rem(i, ZSLOTS)
        if h == 1:
            copy_a(i).wait_recv()
            zsum[zs] += a_recv[i].astype(jnp.float32)
        else:
            take(h - 1, i)
        if h == ZN:
            return

        @pl.when(jnp.logical_and(has_above, z <= h - 1))
        def _():
            reuse(lambda k: copy_u(h, k), i)
            zu_send[h - 1, s] = zsum[zs, rows((z + ZN - h) * BLOCK, BLOCK), :].astype(jnp.bfloat16)
            copy_u(h, i).start()

        @pl.when(jnp.logical_and(has_below, z >= ZN - h))
        def _():
            reuse(lambda k: copy_v(h, k), i)
            zd_send[h - 1, s] = zsum[zs, rows((z - ZN + h) * BLOCK, BLOCK), :].astype(jnp.bfloat16)
            copy_v(h, i).start()

    def take(h, i):
        zs = lax.rem(i, ZSLOTS)

        @pl.when(jnp.logical_and(has_below, z <= h))
        def _():
            copy_u(h, i).wait_recv()
            zsum[zs, rows((z + ZN - 1 - h) * BLOCK, BLOCK), :] += zu_recv[h - 1, i].astype(jnp.float32)

        @pl.when(jnp.logical_and(has_above, z >= ZN - 1 - h))
        def _():
            copy_v(h, i).wait_recv()
            zsum[zs, rows((z - ZN + 1 + h) * BLOCK, BLOCK), :] += zd_recv[h - 1, i].astype(jnp.float32)

    def step_c(i):
        s, zs = lax.rem(i, SLOTS), lax.rem(i, ZSLOTS)
        take(ZN - 1, i)
        reuse(copy_c, i)
        c_send[s] = zsum[zs, rows(z * BLOCK + (1 - third) * PIECE, PIECE), :].astype(jnp.bfloat16)
        copy_c(i).start()
        c_keep[s] = zsum[zs, rows(z * BLOCK + third * PIECE, PIECE), :]

    def step_g0(i):
        s = lax.rem(i, SLOTS)
        copy_c(i).wait_recv()
        total = c_keep[s] + c_recv[i].astype(jnp.float32)
        n, cols = spot(i)
        out[n, rows(base_c + third * PIECE, PIECE), cols] = total.astype(jnp.bfloat16)
        copy_gc(i).start()

    def spread(k, i):
        if k == 1:
            copy_gc(i, False).wait_recv()
        else:
            arrive(k - 1, i)

        @pl.when(jnp.logical_and(has_above, z >= k - 1))
        def _():
            copy_gu(k, i, z - k + 1).start()

        @pl.when(jnp.logical_and(has_below, z <= ZN - k))
        def _():
            copy_gv(k, i, z + k - 1).start()

    def arrive(k, i):
        @pl.when(z >= k)
        def _():
            copy_gu(k, i, z - k).wait_recv()

        @pl.when(z <= ZN - 1 - k)
        def _():
            copy_gv(k, i, z + k).wait_recv()

    def step_g4(i):
        arrive(ZN - 1, i)
        copy_ga(i).start()

    def step_g5(i):
        copy_ga(i, False).wait_recv()
        copy_gd(i).start()

    steps = dict(
        a=step_a,
        z1=lambda i: hop(1, i),
        z2=lambda i: hop(2, i),
        z3=lambda i: hop(3, i),
        c=step_c,
        g0=step_g0,
        g1=lambda i: spread(1, i),
        g2=lambda i: spread(2, i),
        g3=lambda i: spread(3, i),
        g4=step_g4,
        g5=step_g5,
    )
    order = sorted(steps, key=lambda name: -AT[name])

    def run(u, half):
        for name in order:
            if AT[name] % 2 == half:
                i = u - AT[name] // 2

                @pl.when(jnp.logical_and(i >= 0, i < TILES))
                def _():
                    steps[name](i)

    def term(n, gs, mine, start, size):
        cols = slice(mine * HALF + start, mine * HALF + start + size)
        return lax.dot_general(av[n, :, cols], gv[gs], DN, preferred_element_type=jnp.float32)

    def compute(u, half):
        n, gs = lax.div(u, PER), lax.rem(u, GSLOTS)
        if half == 0:

            @pl.when(u + 2 < TILES)
            def _():
                load_g(u + 2).start()

            @pl.when(u == 2)
            def _():
                load_a(0).start()
                load_a(1).start()

            @pl.when(u > 0)
            def _():
                load_g(u).wait()

            @pl.when(u == PER)
            def _():
                load_a(0).wait()
                load_a(1).wait()

            reuse(copy_d, u)

        @pl.when(u > 0)
        def _():
            start, size = half * HALF // 2, HALF // 2
            d_send[lax.rem(u, SLOTS), start : start + size] = term(n, gs, 0, start, size).astype(jnp.bfloat16)
            own[lax.rem(u, 2), start : start + size] = term(n, gs, 1, start, size)

        if half == 1:
            copy_d(u).start()

    def loop(u, carry):
        for half in range(2):
            run(u, half)
            pl.when(u < TILES)(lambda half=half: compute(u, half))
        return carry

    lax.fori_loop(0, TILES + max(AT.values()) // 2, loop, 0)

    def finish_staged(i, carry):
        copy_d(i).wait_send()
        copy_a(i).wait_send()
        copy_c(i).wait_send()
        for h in range(1, ZN):

            @pl.when(jnp.logical_and(has_above, z <= h - 1))
            def _():
                copy_u(h, i).wait_send()

            @pl.when(jnp.logical_and(has_below, z >= ZN - h))
            def _():
                copy_v(h, i).wait_send()

        return carry

    lax.fori_loop(TILES - SLOTS, TILES, finish_staged, 0)

    def all_of(size, send, recv, dev):
        ref = out.at[:, 0:size, :]
        return remote(ref, ref, send, recv, dev)

    all_of(PIECE, gcs, gdr, third_peer).wait_send()
    all_of(QUARTER, gas, gdr, first_peer).wait_send()
    for k in range(1, ZN):

        @pl.when(jnp.logical_and(has_above, z >= k - 1))
        def _():
            all_of(BLOCK, gus.at[k - 1], gdr, above).wait_send()

        @pl.when(jnp.logical_and(has_below, z <= ZN - k))
        def _():
            all_of(BLOCK, gvs.at[k - 1], gdr, below).wait_send()

    all_of(HALF, gds, gdr, partner).wait()


def put(sums, out, sem):
    copies = []
    for k in range(MATS * PUTS):
        part = (k // PUTS, pl.ds(k % PUTS * (D // PUTS), D // PUTS))
        copies.append(pltpu.make_async_copy(sums.at[part], out.at[part], sem.at[k]))
        copies[-1].start()
    for copy in copies:
        copy.wait()


def solution(mesh):
    bf16, f32 = jnp.bfloat16, jnp.float32

    def step(a, g):
        dma = pltpu.SemaphoreType.DMA
        one, three = dma((SLOTS,)), dma((ZN - 1, SLOTS))
        scratch = [
            pltpu.VMEM((MATS, TOKENS, D), bf16),
            pltpu.VMEM((GSLOTS, TOKENS, COLS), bf16),
            pltpu.VMEM((2, HALF, COLS), f32),
            pltpu.VMEM((SLOTS, HALF, COLS), bf16),
            pltpu.VMEM((TILES, HALF, COLS), bf16),
            pltpu.VMEM((SLOTS, QUARTER, COLS), bf16),
            pltpu.VMEM((TILES, QUARTER, COLS), bf16),
            pltpu.VMEM((ZSLOTS, QUARTER, COLS), f32),
            pltpu.VMEM((ZN - 1, SLOTS, BLOCK, COLS), bf16),
            pltpu.VMEM((ZN - 1, SLOTS, BLOCK, COLS), bf16),
            pltpu.VMEM((ZN - 1, TILES, BLOCK, COLS), bf16),
            pltpu.VMEM((ZN - 1, TILES, BLOCK, COLS), bf16),
            pltpu.VMEM((SLOTS, PIECE, COLS), bf16),
            pltpu.VMEM((SLOTS, PIECE, COLS), f32),
            pltpu.VMEM((TILES, PIECE, COLS), bf16),
            dma((2,)),
            dma((GSLOTS,)),
            dma((3, PIECES)),
        ]
        scratch += [one] * 4 + [three] * 4 + [one] * 2
        hops = dma((ZN - 1,))
        scratch += [dma, one, hops, three, hops, three, dma, dma((LATE,)), dma, dma]
        sums = pl.pallas_call(
            kernel,
            out_shape=pltpu.VMEM((MATS, D, FF), bf16),
            in_specs=[pl.BlockSpec(memory_space=pl.ANY)] * 2,
            out_specs=pl.BlockSpec(memory_space=pltpu.VMEM),
            scratch_shapes=scratch,
            compiler_params=pltpu.CompilerParams(
                collective_id=0, has_side_effects=True, vmem_limit_bytes=48 * 2**20
            ),
        )(a, g)
        return pl.pallas_call(
            put,
            out_shape=jax.ShapeDtypeStruct((MATS, D, FF), bf16),
            in_specs=[pl.BlockSpec(memory_space=pltpu.VMEM)],
            out_specs=pl.BlockSpec(memory_space=pl.ANY),
            scratch_shapes=[dma((MATS * PUTS,))],
            compiler_params=pltpu.CompilerParams(vmem_limit_bytes=2**20),
        )(sums)

    return jax.shard_map(
        step,
        mesh=mesh,
        in_specs=(P(("rep", "dp")), P(("rep", "dp"))),
        out_specs=P("rep"),
        check_vma=False,
    )
```

```python
import jax
import jax.numpy as jnp
from jax import lax
from jax.experimental import pallas as pl
from jax.experimental.pallas import tpu as pltpu
from jax.sharding import PartitionSpec as P

MESH = pl.DeviceIdType.MESH
MATS, TOKENS, D, FF = 2, 4096, 1024, 3328
COLS = 256
PER = FF // COLS
TILES = MATS * PER
HALF = D // 2
PIECES = 4
STEP = TOKENS // PIECES
QUARTER, BLOCK, PIECE = HALF // 2, HALF // 8, HALF // 16
ZN = 4
GSLOTS = 3
SLOTS = 6
LATE = 12
ZSLOTS = 9
PUTS = 8
AT = dict(a=3, z1=7, z2=10, z3=13, c=16, g0=19, g1=22, g2=25, g3=29, g4=32, g5=40)
DN = (((0,), (0,)), ((), ()))


def kernel(
    a_hbm, g_hbm, out, av, gv, own, d_send, d_recv, a_send, a_recv, zsum, zu_send, zd_send, zu_recv, zd_recv,
    c_send, c_keep, c_recv, a_sem, g_sem, first_sem, ds, dr, xs, xr, us, ur, vs, vr, cs, cr,
    gcs, gcr, gus, gur, gvs, gvr, gas, gar, gds, gdr,
):
    rep, me = lax.axis_index("rep"), lax.axis_index("dp")
    c, z = lax.rem(me, 2), lax.rem(lax.div(me, 2), ZN)
    y, x = lax.rem(lax.div(me, 8), 2), lax.div(me, 16)
    first = jnp.where(c == 0, x, y)
    third = jnp.where(c == 0, y, x)
    over_x, over_y = me + 16 * (1 - 2 * x), me + 8 * (1 - 2 * y)
    first_peer = jnp.where(c == 0, over_x, over_y)
    third_peer = jnp.where(c == 0, over_y, over_x)
    partner, above, below = me + 1 - 2 * c, me + 2, me - 2
    has_above, has_below = z < ZN - 1, z > 0

    def remote(src, dst, send, recv, dev):
        return pltpu.make_async_remote_copy(
            src_ref=src, dst_ref=dst, send_sem=send, recv_sem=recv, device_id=(rep, dev), device_id_type=MESH
        )

    def load_g(u):
        n, j = lax.div(u, PER), lax.rem(u, PER)
        s = lax.rem(u, GSLOTS)
        return pltpu.make_async_copy(
            g_hbm.at[0, n, :, pl.ds(pl.multiple_of(j * COLS, COLS), COLS)], gv.at[s], g_sem.at[s]
        )

    def load_a(k):
        cols = pl.ds(pl.multiple_of((1 - c if k == 0 else c) * HALF, HALF), HALF)
        return pltpu.make_async_copy(a_hbm.at[0, 1, :, cols], av.at[1, :, k * HALF : (k + 1) * HALF], a_sem.at[k])

    def load_first(p):
        tokens = pl.ds(pl.multiple_of(p * STEP, STEP), STEP)
        copies = [pltpu.make_async_copy(g_hbm.at[0, 0, tokens, 0:COLS], gv.at[0, tokens, :], first_sem.at[2, p])]
        for k in range(2):
            cols = pl.ds(pl.multiple_of((1 - c if k == 0 else c) * HALF, HALF), HALF)
            copies.append(
                pltpu.make_async_copy(
                    a_hbm.at[0, 0, tokens, cols], av.at[0, tokens, k * HALF : (k + 1) * HALF], first_sem.at[k, p]
                )
            )
        return copies

    for copy in load_first(0) + load_first(1):
        copy.start()

    barrier = pltpu.get_barrier_semaphore()
    for dev in (partner, over_x, over_y):
        pl.semaphore_signal(barrier, inc=1, device_id=(rep, dev), device_id_type=MESH)

    @pl.when(has_above)
    def _():
        pl.semaphore_signal(barrier, inc=1, device_id=(rep, above), device_id_type=MESH)

    @pl.when(has_below)
    def _():
        pl.semaphore_signal(barrier, inc=1, device_id=(rep, below), device_id_type=MESH)


    def rows(start, size):
        return pl.ds(pl.multiple_of(start, size), size)

    own[...] = jnp.zeros_like(own)

    def piece(k, carry):
        for copy in load_first(k):
            copy.wait()

        @pl.when(k + 2 < PIECES)
        def _():
            for copy in load_first(k + 2):
                copy.start()

        @pl.when(k == 1)
        def _():
            load_g(1).start()

        tokens = rows(k * STEP, STEP)
        for slot, mine in ((1, 0), (0, 1)):
            own[slot] += lax.dot_general(
                av[0, tokens, mine * HALF : (mine + 1) * HALF],
                gv[0, tokens, :],
                DN,
                preferred_element_type=jnp.float32,
            )
        return carry

    lax.fori_loop(0, PIECES, piece, 0)
    d_send[0] = own[1].astype(jnp.bfloat16)

    pl.semaphore_wait(barrier, 3 + has_above.astype(jnp.int32) + has_below.astype(jnp.int32))

    def copy_d(i):
        s = lax.rem(i, SLOTS)
        return remote(d_send.at[s], d_recv.at[i], ds.at[s], dr.at[s], partner)

    def copy_a(i):
        s = lax.rem(i, SLOTS)
        return remote(a_send.at[s], a_recv.at[i], xs.at[s], xr.at[s], first_peer)

    def copy_u(h, i):
        s = lax.rem(i, SLOTS)
        return remote(zu_send.at[h - 1, s], zu_recv.at[h - 1, i], us.at[h - 1, s], ur.at[h - 1, s], above)

    def copy_v(h, i):
        s = lax.rem(i, SLOTS)
        return remote(zd_send.at[h - 1, s], zd_recv.at[h - 1, i], vs.at[h - 1, s], vr.at[h - 1, s], below)

    def copy_c(i):
        s = lax.rem(i, SLOTS)
        return remote(c_send.at[s], c_recv.at[i], cs.at[s], cr.at[s], third_peer)

    def spot(i):
        n, j = lax.div(i, PER), lax.rem(i, PER)
        return n, pl.ds(pl.multiple_of(j * COLS, COLS), COLS)

    def place(i, start, size):
        n, cols = spot(i)
        return out.at[n, rows(start, size), cols]

    def shared(i, start, size, send, recv, dev):
        ref = place(i, start, size)
        return remote(ref, ref, send, recv, dev)

    base_a = c * HALF + first * QUARTER
    base_c = base_a + z * BLOCK

    def copy_gc(i, mine=True):
        return shared(i, base_c + (third if mine else 1 - third) * PIECE, PIECE, gcs, gcr.at[lax.rem(i, SLOTS)], third_peer)

    def copy_gu(k, i, block):
        return shared(i, base_a + block * BLOCK, BLOCK, gus.at[k - 1], gur.at[k - 1, lax.rem(i, SLOTS)], above)

    def copy_gv(k, i, block):
        return shared(i, base_a + block * BLOCK, BLOCK, gvs.at[k - 1], gvr.at[k - 1, lax.rem(i, SLOTS)], below)

    def copy_ga(i, mine=True):
        return shared(
            i, c * HALF + (first if mine else 1 - first) * QUARTER, QUARTER, gas, gar.at[lax.rem(i, LATE)], first_peer
        )

    def copy_gd(i, mine=True):
        return shared(i, (c if mine else 1 - c) * HALF, HALF, gds, gdr, partner)

    def reuse(copy, i):
        @pl.when(i >= SLOTS)
        def _():
            copy(i - SLOTS).wait_send()

    def step_a(i):
        s, zs = lax.rem(i, SLOTS), lax.rem(i, ZSLOTS)
        o = lax.rem(i, 2)
        copy_d(i).wait_recv()
        reuse(copy_a, i)
        away, keep = rows((1 - first) * QUARTER, QUARTER), rows(first * QUARTER, QUARTER)
        a_send[s] = (own[o, away, :] + d_recv[i, away, :].astype(jnp.float32)).astype(jnp.bfloat16)
        copy_a(i).start()
        zsum[zs] = own[o, keep, :] + d_recv[i, keep, :].astype(jnp.float32)

    def hop(h, i):
        s, zs = lax.rem(i, SLOTS), lax.rem(i, ZSLOTS)
        if h == 1:
            copy_a(i).wait_recv()
            zsum[zs] += a_recv[i].astype(jnp.float32)
        else:
            take(h - 1, i)
        if h == ZN:
            return

        @pl.when(jnp.logical_and(has_above, z <= h - 1))
        def _():
            reuse(lambda k: copy_u(h, k), i)
            zu_send[h - 1, s] = zsum[zs, rows((z + ZN - h) * BLOCK, BLOCK), :].astype(jnp.bfloat16)
            copy_u(h, i).start()

        @pl.when(jnp.logical_and(has_below, z >= ZN - h))
        def _():
            reuse(lambda k: copy_v(h, k), i)
            zd_send[h - 1, s] = zsum[zs, rows((z - ZN + h) * BLOCK, BLOCK), :].astype(jnp.bfloat16)
            copy_v(h, i).start()

    def take(h, i):
        zs = lax.rem(i, ZSLOTS)

        @pl.when(jnp.logical_and(has_below, z <= h))
        def _():
            copy_u(h, i).wait_recv()
            zsum[zs, rows((z + ZN - 1 - h) * BLOCK, BLOCK), :] += zu_recv[h - 1, i].astype(jnp.float32)

        @pl.when(jnp.logical_and(has_above, z >= ZN - 1 - h))
        def _():
            copy_v(h, i).wait_recv()
            zsum[zs, rows((z - ZN + 1 + h) * BLOCK, BLOCK), :] += zd_recv[h - 1, i].astype(jnp.float32)

    def step_c(i):
        s, zs = lax.rem(i, SLOTS), lax.rem(i, ZSLOTS)
        take(ZN - 1, i)
        reuse(copy_c, i)
        c_send[s] = zsum[zs, rows(z * BLOCK + (1 - third) * PIECE, PIECE), :].astype(jnp.bfloat16)
        copy_c(i).start()
        c_keep[s] = zsum[zs, rows(z * BLOCK + third * PIECE, PIECE), :]

    def step_g0(i):
        s = lax.rem(i, SLOTS)
        copy_c(i).wait_recv()
        total = c_keep[s] + c_recv[i].astype(jnp.float32)
        n, cols = spot(i)
        out[n, rows(base_c + third * PIECE, PIECE), cols] = total.astype(jnp.bfloat16)
        copy_gc(i).start()

    def spread(k, i):
        if k == 1:
            copy_gc(i, False).wait_recv()
        else:
            arrive(k - 1, i)

        @pl.when(jnp.logical_and(has_above, z >= k - 1))
        def _():
            copy_gu(k, i, z - k + 1).start()

        @pl.when(jnp.logical_and(has_below, z <= ZN - k))
        def _():
            copy_gv(k, i, z + k - 1).start()

    def arrive(k, i):
        @pl.when(z >= k)
        def _():
            copy_gu(k, i, z - k).wait_recv()

        @pl.when(z <= ZN - 1 - k)
        def _():
            copy_gv(k, i, z + k).wait_recv()

    def step_g4(i):
        arrive(ZN - 1, i)
        copy_ga(i).start()

    def step_g5(i):
        copy_ga(i, False).wait_recv()
        copy_gd(i).start()

    steps = dict(
        a=step_a,
        z1=lambda i: hop(1, i),
        z2=lambda i: hop(2, i),
        z3=lambda i: hop(3, i),
        c=step_c,
        g0=step_g0,
        g1=lambda i: spread(1, i),
        g2=lambda i: spread(2, i),
        g3=lambda i: spread(3, i),
        g4=step_g4,
        g5=step_g5,
    )
    order = sorted(steps, key=lambda name: AT[name])

    def run(u, half):
        for name in order:
            if AT[name] % 2 == half:
                i = u - AT[name] // 2

                @pl.when(jnp.logical_and(i >= 0, i < TILES))
                def _():
                    steps[name](i)

    def term(n, gs, mine, start, size):
        cols = slice(mine * HALF + start, mine * HALF + start + size)
        return lax.dot_general(av[n, :, cols], gv[gs], DN, preferred_element_type=jnp.float32)

    def compute(u, half):
        n, gs = lax.div(u, PER), lax.rem(u, GSLOTS)
        if half == 0:

            @pl.when(u + 2 < TILES)
            def _():
                load_g(u + 2).start()

            @pl.when(u == 2)
            def _():
                load_a(0).start()
                load_a(1).start()

            @pl.when(u > 0)
            def _():
                load_g(u).wait()

            @pl.when(u == PER)
            def _():
                load_a(0).wait()
                load_a(1).wait()

            reuse(copy_d, u)

        @pl.when(u > 0)
        def _():
            start, size = half * HALF // 2, HALF // 2
            d_send[lax.rem(u, SLOTS), start : start + size] = term(n, gs, 0, start, size).astype(jnp.bfloat16)
            own[lax.rem(u, 2), start : start + size] = term(n, gs, 1, start, size)

        if half == 1:
            copy_d(u).start()

    def loop(u, carry):
        for half in range(2):
            run(u, half)
            pl.when(u < TILES)(lambda half=half: compute(u, half))
        return carry

    lax.fori_loop(0, TILES + max(AT.values()) // 2, loop, 0)

    def finish_staged(i, carry):
        copy_d(i).wait_send()
        copy_a(i).wait_send()
        copy_c(i).wait_send()
        for h in range(1, ZN):

            @pl.when(jnp.logical_and(has_above, z <= h - 1))
            def _():
                copy_u(h, i).wait_send()

            @pl.when(jnp.logical_and(has_below, z >= ZN - h))
            def _():
                copy_v(h, i).wait_send()

        return carry

    lax.fori_loop(TILES - SLOTS, TILES, finish_staged, 0)

    def all_of(size, send, recv, dev):
        ref = out.at[:, 0:size, :]
        return remote(ref, ref, send, recv, dev)

    all_of(PIECE, gcs, gdr, third_peer).wait_send()
    all_of(QUARTER, gas, gdr, first_peer).wait_send()
    for k in range(1, ZN):

        @pl.when(jnp.logical_and(has_above, z >= k - 1))
        def _():
            all_of(BLOCK, gus.at[k - 1], gdr, above).wait_send()

        @pl.when(jnp.logical_and(has_below, z <= ZN - k))
        def _():
            all_of(BLOCK, gvs.at[k - 1], gdr, below).wait_send()

    all_of(HALF, gds, gdr, partner).wait()


def put(sums, out, sem):
    copies = []
    for k in range(MATS * PUTS):
        part = (k // PUTS, pl.ds(k % PUTS * (D // PUTS), D // PUTS))
        copies.append(pltpu.make_async_copy(sums.at[part], out.at[part], sem.at[k]))
        copies[-1].start()
    for copy in copies:
        copy.wait()


def solution(mesh):
    bf16, f32 = jnp.bfloat16, jnp.float32

    def step(a, g):
        dma = pltpu.SemaphoreType.DMA
        one, three = dma((SLOTS,)), dma((ZN - 1, SLOTS))
        scratch = [
            pltpu.VMEM((MATS, TOKENS, D), bf16),
            pltpu.VMEM((GSLOTS, TOKENS, COLS), bf16),
            pltpu.VMEM((2, HALF, COLS), f32),
            pltpu.VMEM((SLOTS, HALF, COLS), bf16),
            pltpu.VMEM((TILES, HALF, COLS), bf16),
            pltpu.VMEM((SLOTS, QUARTER, COLS), bf16),
            pltpu.VMEM((TILES, QUARTER, COLS), bf16),
            pltpu.VMEM((ZSLOTS, QUARTER, COLS), f32),
            pltpu.VMEM((ZN - 1, SLOTS, BLOCK, COLS), bf16),
            pltpu.VMEM((ZN - 1, SLOTS, BLOCK, COLS), bf16),
            pltpu.VMEM((ZN - 1, TILES, BLOCK, COLS), bf16),
            pltpu.VMEM((ZN - 1, TILES, BLOCK, COLS), bf16),
            pltpu.VMEM((SLOTS, PIECE, COLS), bf16),
            pltpu.VMEM((SLOTS, PIECE, COLS), f32),
            pltpu.VMEM((TILES, PIECE, COLS), bf16),
            dma((2,)),
            dma((GSLOTS,)),
            dma((3, PIECES)),
        ]
        scratch += [one] * 4 + [three] * 4 + [one] * 2
        hops = dma((ZN - 1,))
        scratch += [dma, one, hops, three, hops, three, dma, dma((LATE,)), dma, dma]
        sums = pl.pallas_call(
            kernel,
            out_shape=pltpu.VMEM((MATS, D, FF), bf16),
            in_specs=[pl.BlockSpec(memory_space=pl.ANY)] * 2,
            out_specs=pl.BlockSpec(memory_space=pltpu.VMEM),
            scratch_shapes=scratch,
            compiler_params=pltpu.CompilerParams(
                collective_id=0, has_side_effects=True, vmem_limit_bytes=48 * 2**20
            ),
        )(a, g)
        return pl.pallas_call(
            put,
            out_shape=jax.ShapeDtypeStruct((MATS, D, FF), bf16),
            in_specs=[pl.BlockSpec(memory_space=pltpu.VMEM)],
            out_specs=pl.BlockSpec(memory_space=pl.ANY),
            scratch_shapes=[dma((MATS * PUTS,))],
            compiler_params=pltpu.CompilerParams(vmem_limit_bytes=2**20),
        )(sums)

    return jax.shard_map(
        step,
        mesh=mesh,
        in_specs=(P(("rep", "dp")), P(("rep", "dp"))),
        out_specs=P("rep"),
        check_vma=False,
    )
```
